256 devices in a mesh: pipe: 16 (over x_lo, y, core), dp: 16 (over x_hi, z).
Axes of the slice: x: 4 (x_hi: 2, x_lo: 2; x = x_hi * 2 + x_lo), y: 4, z: 8, core: 2. Of those that a mesh axis runs over, the one named last changes fastest.
Arguments:
- inputs: bfloat16 [16, 4096, 4096], P('pipe', 'dp'), may hold values from -6 to 6
- cotangents: bfloat16 [16, 4096, 512], P('pipe', 'dp'), may hold values from -0.09375 to 0.09375
- input_factors: float32 [16, 4096, 256], P('pipe', 'dp'), may hold values from -20 to 20, as said below
- output_factors: float32 [16, 512, 512], P('pipe'), may hold values from -20 to 20, as said below
- input_coupling: float32 [16, 4096, 256], P('pipe', 'dp'), may hold values from -0.375 to 0.375
- output_coupling: float32 [16, 512, 512], P('pipe'), may hold values from -0.25 to 0.25
Outputs:
- update: float32 [16, 4096, 512], P('pipe', 'dp')
The draws below stay inside these ranges and needn't reach their ends.
Inputs may be any that keep to these rules, and one draw needn't show every extreme that they name: Each [256, 256] row block of a layer's input_factors is positive definite. Each layer's output_factors is positive definite.
All inputs are finite; a program needn't handle non-finite values. Where the reference program divides by a largest or mean magnitude, that divisor is 1e-20 or more.
Results may differ from the reference program's by a relative error of at most 0.0003.
Values may be sent and summed in bfloat16 or wider, within the bound.
No kernel may reach another device: no remote copies, remote signals or barrier semaphores. Data moves between devices by JAX's collectives and lax.ppermute only.
A program may use at most 64 MiB of HBM per device.

```python
import math
import jax
import jax.numpy as jnp
from jax import lax

BLOCK = 256
OUTC = 512
NS_ITERS = 2
LAYERS = 16
PANEL = 4096
TOKENS = 4096


def factor_block(key, order):
    key_noise, key_spread = jax.random.split(key)
    samples = jax.random.normal(key_noise, (order, 4 * order), jnp.float32)
    spread = jnp.exp(jax.random.uniform(key_spread, (order,), jnp.float32, 0.0, math.log(3.0)))
    product = jnp.dot(samples, samples.T, precision=lax.Precision.HIGHEST) / (4.0 * order)
    return spread[:, None] * product * spread[None, :]


def input_block(key):
    return factor_block(key, BLOCK)


def output_block(key):
    return factor_block(key, OUTC)


def draw_input_factors(key, part):
    block_count = LAYERS * (PANEL // BLOCK)
    key_list = jax.random.split(jax.random.fold_in(key, 11), block_count)
    stacked = lax.map(input_block, key_list)
    return stacked.reshape(LAYERS, PANEL, BLOCK)


def draw_output_factors(key, part):
    key_list = jax.random.split(jax.random.fold_in(key, 23), LAYERS)
    return lax.map(output_block, key_list)


def strengthened(values, key, source, target, blocks, factor):
    def block_of(axis_at):
        return (jnp.arange(values.shape[axis_at]) // (values.shape[axis_at] // blocks)).reshape((-1,) + (1,) * (values.ndim - 1 - axis_at))

    near = jax.random.permutation(key, blocks)[block_of(target)]
    other_side = (block_of(target) + blocks // 2) % blocks
    return jnp.where((block_of(source) == near) | (block_of(source) == other_side), factor * values, values)


def block_scale(rng, shape, shards, smallest, high):
    factor_of, own = 1.0, jax.random.fold_in(rng, 6)
    for dim, parts in shards:
        steps = jnp.exp(jax.random.uniform(jax.random.fold_in(own, dim), (parts,), jnp.float32, smallest / len(shards), high / len(shards)))
        factor_of = factor_of * jnp.repeat(steps, shape[dim] // parts).reshape([-1 if axis == dim else 1 for axis in range(len(shape))])
    return factor_of


def noise(rng, shape, width, reach, cuts=(), kind=jnp.bfloat16):
    array = width * jax.random.normal(rng, shape, jnp.float32)
    if cuts:
        array = array * block_scale(rng, shape, cuts, -0.22, 0.18)
    return jnp.clip(array, -reach, reach).astype(kind)


def heavy_noise(key, dims, scale, bound, cuts, heavy, kind=jnp.bfloat16):
    array = scale * jax.random.normal(key, dims, jnp.float32)
    if cuts:
        array = array * block_scale(key, dims, cuts, -0.22, 0.18)
    return jnp.clip(strengthened(array, jax.random.fold_in(key, 3), *heavy), -bound, bound).astype(kind)


def setup_inputs(seed: int = 0) -> dict:
    streams_of = jax.random.split(jax.random.key(seed), 7)
    inputs = heavy_noise(streams_of[0], (LAYERS, TOKENS, PANEL), 1.0, 6.0, ((0, 16), (1, 16)), (1, 2, 16, 2.0))
    cotangents = noise(streams_of[1], (LAYERS, TOKENS, OUTC), 0.015625, 0.09375, ((0, 16), (1, 16)))
    input_factors = draw_input_factors(jax.random.fold_in(streams_of[6], 71), 0)
    output_factors = draw_output_factors(jax.random.fold_in(streams_of[6], 71), 0)
    input_coupling = noise(streams_of[4], (LAYERS, PANEL, BLOCK), BLOCK ** -0.5, 0.375, ((0, 16), (1, 16)), jnp.float32)
    output_coupling = noise(streams_of[5], (LAYERS, OUTC, OUTC), OUTC ** -0.5, 0.25, ((0, 16),), jnp.float32)
    return dict(inputs=inputs, cotangents=cotangents, input_factors=input_factors, output_factors=output_factors, input_coupling=input_coupling, output_coupling=output_coupling)


def matmul(left, right):
    return jnp.matmul(left, right, precision=lax.Precision.HIGHEST)


def invert(factor):
    order = factor.shape[-1]
    identity = jnp.eye(order, dtype=jnp.float32)
    bound_value = jnp.max(jnp.sum(jnp.abs(factor), axis=1))
    iterate = identity / bound_value
    for sweep in range(NS_ITERS):
        iterate = matmul(iterate, 2.0 * identity - matmul(factor, iterate))
    return iterate


def layer_gradient(pair):
    activations, cotangent_block = pair
    return lax.dot_general(activations, cotangent_block, (((0,), (0,)), ((), ())), preferred_element_type=jnp.float32)


def reference(inputs, cotangents, input_factors, output_factors, input_coupling, output_coupling):
    blocks = PANEL // BLOCK
    gradient = lax.map(layer_gradient, (inputs, cotangents))
    gradient = gradient.reshape(LAYERS, blocks, BLOCK, OUTC)
    factor_blocks = input_factors.reshape(LAYERS, blocks, BLOCK, BLOCK)
    coupling_blocks = input_coupling.reshape(LAYERS, blocks, BLOCK, BLOCK)
    input_inverse = lax.map(jax.vmap(invert), factor_blocks)
    output_inverse = lax.map(invert, output_factors)
    highest = lax.Precision.HIGHEST
    following = jnp.concatenate([gradient[1:], jnp.zeros_like(gradient[:1])], axis=0)
    mixed = jnp.einsum("lbij,lbjk->lbik", coupling_blocks, following, precision=highest)
    mixed = jnp.einsum("lbik,lmk->lbim", mixed, output_coupling, precision=highest)
    coupled = gradient - mixed
    scaled = jnp.einsum("lbij,lbjk->lbik", input_inverse, coupled, precision=highest)
    scaled = jnp.einsum("lbik,lkm->lbim", scaled, output_inverse, precision=highest)
    carried = jnp.einsum("lbji,lbjk->lbik", coupling_blocks, scaled, precision=highest)
    carried = jnp.einsum("lbik,lkm->lbim", carried, output_coupling, precision=highest)
    earlier = jnp.concatenate([jnp.zeros_like(carried[:1]), carried[:-1]], axis=0)
    update = scaled - earlier
    return update.reshape(LAYERS, PANEL, OUTC)
```

```python
import jax
import jax.numpy as jnp
from jax import lax
from jax.sharding import PartitionSpec as P

HIGH = lax.Precision.HIGH
AXES = ("pipe", "dp")
BLOCK = 256
RING = 8


def permutation(move):
    pairs = []
    for layer in range(16):
        for half in range(2):
            for place in range(RING):
                to_half, to_place = move(layer % 2, half, place)
                pairs.append((layer * 16 + half * RING + place, layer * 16 + to_half % 2 * RING + to_place % RING))
    return pairs


ACROSS = permutation(lambda core, half, place: (half + 1, place))
LONG = permutation(lambda core, half, place: (half, place + (1 if core == 0 else -1)))
SHORT = permutation(lambda core, half, place: (half, place - (1 if core == 0 else -1)))


def passed_along(value, steps):
    first, last = (max(0, -steps), min(16, 16 - steps))
    return lax.ppermute(value, "pipe", [(source, source + steps) for source in range(first, last)])


def mm(left, right):
    return jnp.matmul(left, right, precision=HIGH)


def invert(factor):
    order = factor.shape[-1]
    identity = jnp.eye(order, dtype=jnp.float32)
    scale = 1.0 / jnp.max(jnp.sum(jnp.abs(factor), axis=1))
    iterate = scale * (2.0 * identity - scale * factor)
    return mm(iterate, 2.0 * identity - mm(factor, iterate))


def contract_tokens(left, right):
    return lax.dot_general(left, right, (((0,), (0,)), ((), ())), preferred_element_type=jnp.float32)


def shards(inputs, cotangents, input_factors, output_factors, input_coupling, output_coupling):
    rows = inputs[0]
    cots = cotangents[0]
    spot = lax.axis_index("dp")
    half, place = spot // RING, spot % RING
    sign = 1 - 2 * (lax.axis_index("pipe") % 2)

    def piece(of_half, offset):
        start = of_half * (RING * BLOCK) + (place + sign * offset + RING) % RING * BLOCK
        return lax.dynamic_slice_in_dim(rows, start, BLOCK, axis=1)

    groups = ((4,), (-3, 3), (-2, 2), (-1, 1, 0))
    theirs = {}
    their_cots = None
    for index, group in enumerate(groups):
        message = [piece(1 - half, offset) for offset in group]
        if index == 0:
            message.append(cots)
        arrived = lax.ppermute(jnp.concatenate(message, axis=1), AXES, ACROSS)
        for at, offset in enumerate(group):
            theirs[offset] = arrived[:, at * BLOCK : (at + 1) * BLOCK]
        if index == 0:
            their_cots = arrived[:, BLOCK:]

    def partial(offset):
        return contract_tokens(piece(half, offset), cots) + contract_tokens(theirs[offset], their_cots)

    coupling = input_coupling[0]
    coupling_out = output_coupling[0]
    left = invert(input_factors[0])
    right = invert(output_factors[0])
    left_next = mm(left, coupling)
    right_next = mm(coupling_out.T, right)
    left_back = mm(coupling.T, left)
    right_back = mm(right, coupling_out)
    left_own = passed_along(mm(coupling.T, left_next), 1)
    right_own = passed_along(mm(right_next, coupling_out), 1)

    long_way = partial(4)
    short_way = partial(-3)
    for step in range(4):
        long_way = lax.ppermute(long_way, AXES, LONG) + partial(3 - step)
        if step < 2:
            short_way = lax.ppermute(short_way, AXES, SHORT) + partial(step - 2)
        elif step == 2:
            short_way = lax.ppermute(short_way, AXES, SHORT)
    gradient = long_way + short_way

    following = passed_along(gradient, -1)
    back = passed_along(mm(mm(left_back, gradient), right_back), 1)
    mine = mm(mm(left, gradient), right) + mm(mm(left_own, gradient), right_own)
    update = mine - mm(mm(left_next, following), right_next) - back
    return update[None]


def solution(mesh):
    in_specs = (
        P("pipe", "dp", None),
        P("pipe", "dp", None),
        P("pipe", "dp", None),
        P("pipe", None, None),
        P("pipe", "dp", None),
        P("pipe", None, None),
    )
    out_specs = P("pipe", "dp", None)
    return jax.shard_map(shards, mesh=mesh, in_specs=in_specs, out_specs=out_specs, check_vma=False)
```

```python
import jax
import jax.numpy as jnp
from jax import lax
from jax.experimental import pallas as pl
from jax.experimental.pallas import tpu as pltpu
from jax.sharding import PartitionSpec as P


AXES = ("pipe", "dp")
BLOCK = 256
OUT = 512
TOKENS = 256
VMEM = 12 << 20
RING = 8


def permutation(move):
    pairs = []
    for layer in range(16):
        for half in range(2):
            for place in range(RING):
                to_half, to_place = move(layer % 2, half, place)
                pairs.append((layer * 16 + half * RING + place, layer * 16 + to_half % 2 * RING + to_place % RING))
    return pairs


ACROSS = permutation(lambda core, half, place: (half + 1, place))
LONG = permutation(lambda core, half, place: (half, place + (1 if core == 0 else -1)))
SHORT = permutation(lambda core, half, place: (half, place - (1 if core == 0 else -1)))


def passed_along(value, steps):
    first, last = (max(0, -steps), min(16, 16 - steps))
    return lax.ppermute(value, "pipe", [(source, source + steps) for source in range(first, last)])


def mm(left, right, dim=1):
    dims = (((dim,), (0,)), ((), ()))

    def halves(value):
        high = value.astype(jnp.bfloat16)
        return high, (value - high.astype(jnp.float32)).astype(jnp.bfloat16)

    def dot(one, two):
        return lax.dot_general(one, two, dims, preferred_element_type=jnp.float32)

    (left_high, left_low), (right_high, right_low) = halves(left), halves(right)
    return dot(left_high, right_high) + (dot(left_high, right_low) + dot(left_low, right_high))


def invert(factor):
    shape = factor.shape
    twice = jnp.where(lax.broadcasted_iota(jnp.int32, shape, 0) == lax.broadcasted_iota(jnp.int32, shape, 1), 2.0, 0.0)
    scale = 1.0 / jnp.max(jnp.sum(jnp.abs(factor), axis=1, keepdims=True), axis=0, keepdims=True)
    iterate = scale * (twice - scale * factor)
    return mm(iterate, twice - mm(factor, iterate))


def local(body, flops, shapes, *operands):
    def kernel(*refs):
        results = body(*[ref[...] for ref in refs[: len(operands)]])
        for ref, result in zip(refs[len(operands) :], results):
            ref[...] = result

    return pl.pallas_call(
        kernel,
        out_shape=[jax.ShapeDtypeStruct(shape, jnp.float32) for shape in shapes],
        cost_estimate=pl.CostEstimate(flops=flops, transcendentals=0, bytes_accessed=1 << 20),
        compiler_params=pltpu.CompilerParams(vmem_limit_bytes=VMEM),
    )(*operands)


def contract_tokens(left, right):
    return lax.dot_general(left, right, (((0,), (0,)), ((), ())), preferred_element_type=jnp.float32)


def shards(inputs, cotangents, input_factors, output_factors, input_coupling, output_coupling):
    return whole(inputs[0], cotangents[0], input_factors[0], output_factors[0], input_coupling[0], output_coupling[0])[None]


def sent(value, pairs):
    return lax.ppermute(value, AXES, pairs)


def after(value, *events):
    return lax.optimization_barrier((value, *events))[0]


def whole(rows, cots, factor_in, factor_out, coupling, coupling_out):
    def gather(*lists):
        widths = [sum(OUT if block is None else BLOCK for block in blocks) for blocks in lists]
        count = sum(len(blocks) for blocks in lists)

        def kernel(rows_ref, cots_ref, *refs):
            outs, sems = refs[: len(lists)], refs[len(lists)]
            spot = lax.axis_index("dp")
            half, place = spot // RING, spot % RING
            sign = 1 - 2 * (lax.axis_index("pipe") % 2)
            copies = []
            for out, blocks in zip(outs, lists):
                at = 0
                for block in blocks:
                    if block is None:
                        source, width = cots_ref, OUT
                    else:
                        own, offset = block
                        start = (half if own else 1 - half) * (RING * BLOCK) + (place + sign * offset + RING) % RING * BLOCK
                        source, width = rows_ref.at[:, pl.ds(pl.multiple_of(start, BLOCK), BLOCK)], BLOCK
                    copies.append(pltpu.make_async_copy(source, out.at[:, at : at + width], sems.at[len(copies)]))
                    at += width
            for copy in copies:
                copy.start()
            for copy in copies:
                copy.wait()

        return pl.pallas_call(
            kernel,
            out_shape=[jax.ShapeDtypeStruct((TOKENS, width), jnp.bfloat16) for width in widths],
            in_specs=[pl.BlockSpec(memory_space=pltpu.HBM)] * 2,
            out_specs=[pl.BlockSpec(memory_space=pltpu.VMEM) for _ in widths],
            scratch_shapes=[pltpu.SemaphoreType.DMA((count,))],
            cost_estimate=pl.CostEstimate(flops=10**8, transcendentals=0, bytes_accessed=2 * 512 * sum(widths)),
            compiler_params=pltpu.CompilerParams(vmem_limit_bytes=VMEM),
        )(pltpu.with_memory_space_constraint(rows, pltpu.HBM), pltpu.with_memory_space_constraint(cots, pltpu.HBM))

    groups = ((4,), (-3, 3), (-2, 2), (-1, 1, 0))
    (message_0,) = gather([(False, 4), None])
    arrived = [sent(message_0, ACROSS)]
    message_1, message_2, message_3, *own_rows = gather(
        *[[(False, offset) for offset in group] for group in groups[1:]],
        *[[(True, offset) for offset in group] for group in groups],
    )
    for message in (message_1, message_2, message_3):
        arrived.append(sent(message, ACROSS))

    def partials(index):
        count = len(groups[index])

        def kernel(own_ref, cots_ref, first_ref, *refs):
            their_ref, outs = (refs[0], refs[1:]) if index else (first_ref, refs)
            their_cots = first_ref[:, BLOCK:]
            for at, out in enumerate(outs):
                cut = slice(at * BLOCK, (at + 1) * BLOCK)
                out[...] = contract_tokens(own_ref[:, cut], cots_ref[...]) + contract_tokens(their_ref[:, cut], their_cots)

        operands = (own_rows[index], cots, arrived[0]) + ((arrived[index],) if index else ())
        return pl.pallas_call(
            kernel,
            out_shape=[jax.ShapeDtypeStruct((BLOCK, OUT), jnp.float32)] * count,
            cost_estimate=pl.CostEstimate(flops=count * 4 * BLOCK * BLOCK * OUT, transcendentals=0, bytes_accessed=count << 19),
            compiler_params=pltpu.CompilerParams(vmem_limit_bytes=VMEM),
        )(*operands)

    partial = {}
    for index, group in enumerate(groups):
        for offset, value in zip(group, partials(index)):
            partial[offset] = value

    def total(*values):
        return local(lambda first, *rest: (sum(rest, first),), 10**6, [(BLOCK, OUT)], *values)[0]

    def hop(value, pairs, offset):
        return total(sent(value, pairs), partial[offset])

    long_0 = partial[4]
    short_0 = partial[-3]
    long_1 = hop(long_0, LONG, 3)
    short_1 = hop(short_0, SHORT, -2)
    long_2 = hop(long_1, LONG, 2)
    short_2 = hop(short_1, SHORT, -1)
    long_3 = hop(long_2, LONG, 1)
    short_3 = sent(short_2, SHORT)
    long_4 = sent(long_3, LONG)
    gradient = total(long_4, short_3, partial[0])

    square, wide, full = (BLOCK, BLOCK), (BLOCK, OUT), (OUT, OUT)

    def left_side(factor, coupling):
        left = invert(factor)
        left_next = mm(left, coupling)
        left_own = mm(coupling, left_next, 0)
        packed = jnp.concatenate([left_own[: BLOCK // 2], left_own[BLOCK // 2 :]], axis=1)
        return left, left_next, mm(coupling, left, 0), packed

    def right_side(coupling_out, right, packed):
        right_next = mm(coupling_out, right, 0)
        return right_next, jnp.concatenate([mm(right_next, coupling_out), packed], axis=0)

    def own_terms(gradient, left, right, weights):
        left_own = jnp.concatenate([weights[OUT:, :BLOCK], weights[OUT:, BLOCK:]], axis=0)
        return (mm(mm(left, gradient), right) + mm(mm(left_own, gradient), weights[:OUT]),)

    def product(left, value, right):
        return (mm(mm(left, value), right),)

    left, left_next, left_back, packed = local(left_side, 10**9, [square, square, square, (BLOCK // 2, OUT)], factor_in, coupling)
    (right,) = local(lambda factor: (invert(factor),), 2 * 10**9, [full], after(factor_out, long_1))
    right_next, weights = local(right_side, 2 * 10**9, [full, (OUT + BLOCK // 2, OUT)], coupling_out, after(right, long_2), packed)
    (right_back,) = local(lambda right, out: (mm(right, out),), 10**9, [full], after(right, long_3), coupling_out)
    weights = passed_along(weights, 1)
    following = passed_along(gradient, -1)
    (passed,) = local(product, 10**9, [wide], left_back, gradient, right_back)
    back = passed_along(passed, 1)
    (mine,) = local(own_terms, 2 * 10**9, [wide], gradient, left, right, weights)
    (mine,) = local(
        lambda mine, *rest: (mine - product(*rest)[0],), 10**9, [wide], mine, left_next, following, right_next
    )
    return mine - back


def solution(mesh):
    in_specs = (
        P("pipe", "dp", None),
        P("pipe", "dp", None),
        P("pipe", "dp", None),
        P("pipe", None, None),
        P("pipe", "dp", None),
        P("pipe", None, None),
    )
    out_specs = P("pipe", "dp", None)
    return jax.shard_map(shards, mesh=mesh, in_specs=in_specs, out_specs=out_specs, check_vma=False)
```

```python
import jax
import jax.numpy as jnp
from jax import lax
from jax.experimental import pallas as pl
from jax.experimental.pallas import tpu as pltpu
from jax.sharding import PartitionSpec as P


AXES = ("pipe", "dp")
BLOCK = 256
OUT = 512
TOKENS = 256
VMEM = 12 << 20
RING = 8


def permutation(move):
    pairs = []
    for layer in range(16):
        for half in range(2):
            for place in range(RING):
                to_half, to_place = move(layer % 2, half, place)
                pairs.append((layer * 16 + half * RING + place, layer * 16 + to_half % 2 * RING + to_place % RING))
    return pairs


ACROSS = permutation(lambda core, half, place: (half + 1, place))
LONG = permutation(lambda core, half, place: (half, place + (1 if core == 0 else -1)))
SHORT = permutation(lambda core, half, place: (half, place - (1 if core == 0 else -1)))


def passed_along(value, steps):
    first, last = (max(0, -steps), min(16, 16 - steps))
    return lax.ppermute(value, "pipe", [(source, source + steps) for source in range(first, last)])


def mm(left, right, dim=1):
    dims = (((dim,), (0,)), ((), ()))

    def halves(value):
        high = value.astype(jnp.bfloat16)
        return high, (value - high.astype(jnp.float32)).astype(jnp.bfloat16)

    def dot(one, two):
        return lax.dot_general(one, two, dims, preferred_element_type=jnp.float32)

    (left_high, left_low), (right_high, right_low) = halves(left), halves(right)
    return dot(left_high, right_high) + (dot(left_high, right_low) + dot(left_low, right_high))


def invert(factor):
    shape = factor.shape
    twice = jnp.where(lax.broadcasted_iota(jnp.int32, shape, 0) == lax.broadcasted_iota(jnp.int32, shape, 1), 2.0, 0.0)
    scale = 1.0 / jnp.max(jnp.sum(jnp.abs(factor), axis=1, keepdims=True), axis=0, keepdims=True)
    iterate = scale * (twice - scale * factor)
    return mm(iterate, twice - mm(factor, iterate))


def local(body, flops, shapes, *operands):
    def kernel(*refs):
        results = body(*[ref[...] for ref in refs[: len(operands)]])
        for ref, result in zip(refs[len(operands) :], results):
            ref[...] = result

    return pl.pallas_call(
        kernel,
        out_shape=[jax.ShapeDtypeStruct(shape, jnp.float32) for shape in shapes],
        cost_estimate=pl.CostEstimate(flops=flops, transcendentals=0, bytes_accessed=1 << 20),
        compiler_params=pltpu.CompilerParams(vmem_limit_bytes=VMEM),
    )(*operands)


def contract_tokens(left, right):
    return lax.dot_general(left, right, (((0,), (0,)), ((), ())), preferred_element_type=jnp.float32)


def shards(inputs, cotangents, input_factors, output_factors, input_coupling, output_coupling):
    return whole(inputs[0], cotangents[0], input_factors[0], output_factors[0], input_coupling[0], output_coupling[0])[None]


def sent(value, pairs):
    return lax.ppermute(value, AXES, pairs)


def after(value, *events):
    return lax.optimization_barrier((value, *events))[0]


def whole(rows, cots, factor_in, factor_out, coupling, coupling_out):
    def gather(*lists):
        widths = [BLOCK * len(blocks) for blocks in lists]
        count = sum(len(blocks) for blocks in lists)

        def kernel(rows_ref, cots_ref, *refs):
            outs, sems = refs[: len(lists)], refs[len(lists)]
            spot = lax.axis_index("dp")
            half, place = spot // RING, spot % RING
            sign = 1 - 2 * (lax.axis_index("pipe") % 2)
            copies = []
            for out, blocks in zip(outs, lists):
                at = 0
                for block in blocks:
                    if isinstance(block, int):
                        source, width = cots_ref.at[:, block * BLOCK : (block + 1) * BLOCK], BLOCK
                    else:
                        own, offset = block
                        start = (half if own else 1 - half) * (RING * BLOCK) + (place + sign * offset + RING) % RING * BLOCK
                        source, width = rows_ref.at[:, pl.ds(pl.multiple_of(start, BLOCK), BLOCK)], BLOCK
                    copies.append(pltpu.make_async_copy(source, out.at[:, at : at + width], sems.at[len(copies)]))
                    at += width
            for copy in copies:
                copy.start()
            for copy in copies:
                copy.wait()

        return pl.pallas_call(
            kernel,
            out_shape=[jax.ShapeDtypeStruct((TOKENS, width), jnp.bfloat16) for width in widths],
            in_specs=[pl.BlockSpec(memory_space=pltpu.HBM)] * 2,
            out_specs=[pl.BlockSpec(memory_space=pltpu.VMEM) for _ in widths],
            scratch_shapes=[pltpu.SemaphoreType.DMA((count,))],
            cost_estimate=pl.CostEstimate(flops=10**8, transcendentals=0, bytes_accessed=2 * 512 * sum(widths)),
            compiler_params=pltpu.CompilerParams(vmem_limit_bytes=VMEM),
        )(pltpu.with_memory_space_constraint(rows, pltpu.HBM), pltpu.with_memory_space_constraint(cots, pltpu.HBM))

    groups = ((4,), (-3,), (3, -2), (2, -1), (1, 0))
    (message,) = gather([(False, 4), 0])
    arrived = [sent(message, ACROSS)]
    *messages, own_0, own_1, own_2, own_3, own_4 = gather(
        [1, (False, -3)],
        *[[(False, offset) for offset in group] for group in groups[2:]],
        *[[(True, offset) for offset in group] for group in groups],
    )
    for index, message in enumerate(messages, 1):
        arrived.append(sent(message, ACROSS))

    def sums(mine, cots, theirs, their_cots):
        return contract_tokens(mine, cots) + contract_tokens(theirs, their_cots)

    def first(mine, cots, zero):
        return (sums(mine, cots[:, :BLOCK], zero[:, :BLOCK], zero[:, BLOCK:]),)

    def second(mine_0, mine_1, cots, zero, one):
        near, far = zero[:, BLOCK:], one[:, :BLOCK]
        return (
            sums(mine_0, cots[:, BLOCK:], zero[:, :BLOCK], far),
            sums(mine_1, cots[:, :BLOCK], one[:, BLOCK:], near),
            sums(mine_1, cots[:, BLOCK:], one[:, BLOCK:], far),
        )

    def later(mine, cots, zero, one, theirs):
        return tuple(
            sums(mine[:, at : at + BLOCK], cots[:, part * BLOCK : (part + 1) * BLOCK], theirs[:, at : at + BLOCK], their_cots)
            for at in (0, BLOCK)
            for part, their_cots in enumerate((zero[:, BLOCK:], one[:, :BLOCK]))
        )

    partial = {}
    tile, work = (BLOCK, BLOCK), 4 * BLOCK**3
    partial[4, 0] = local(first, work, [tile], own_0, cots, arrived[0])[0]
    partial[4, 1], partial[-3, 0], partial[-3, 1] = local(
        second, 3 * work, [tile] * 3, own_0, own_1, cots, arrived[0], arrived[1]
    )
    for index, mine in ((2, own_2), (3, own_3), (4, own_4)):
        values = local(later, 4 * work, [tile] * 4, mine, cots, arrived[0], arrived[1], arrived[index])
        for at, offset in enumerate(groups[index]):
            partial[offset, 0], partial[offset, 1] = values[2 * at : 2 * at + 2]

    def hop(value, pairs, offset, part):
        value = sent(value, pairs)
        return local(lambda one, two: (one + two,), 10**6, [tile], value, partial[offset, part])[0]

    long_way = [partial[4, 0], partial[4, 1]]
    short_way = [partial[-3, 0], partial[-3, 1]]
    marks = []
    for long_next, short_next in ((3, -2), (2, -1), (1, None)):
        for part in range(2):
            long_way[part] = hop(long_way[part], LONG, long_next, part)
        for part in range(2):
            if short_next is None:
                short_way[part] = sent(short_way[part], SHORT)
            else:
                short_way[part] = hop(short_way[part], SHORT, short_next, part)
        marks.append(long_way[1])
    long_1, long_2, long_3 = marks
    long_way = [sent(long_way[part], LONG) for part in range(2)]

    def whole_gradient(*values):
        return (jnp.concatenate([values[part] + values[2 + part] + values[4 + part] for part in range(2)], axis=1),)

    (gradient,) = local(whole_gradient, 10**6, [(BLOCK, OUT)], *long_way, *short_way, partial[0, 0], partial[0, 1])

    square, wide, full = (BLOCK, BLOCK), (BLOCK, OUT), (OUT, OUT)

    def left_side(factor, coupling):
        left = invert(factor)
        left_next = mm(left, coupling)
        left_own = mm(coupling, left_next, 0)
        packed = jnp.concatenate([left_own[: BLOCK // 2], left_own[BLOCK // 2 :]], axis=1)
        return left, left_next, mm(coupling, left, 0), packed

    def right_side(coupling_out, right, packed):
        right_next = mm(coupling_out, right, 0)
        return right_next, jnp.concatenate([mm(right_next, coupling_out), packed], axis=0)

    def own_terms(gradient, left, right, weights):
        left_own = jnp.concatenate([weights[OUT:, :BLOCK], weights[OUT:, BLOCK:]], axis=0)
        return (mm(mm(left, gradient), right) + mm(mm(left_own, gradient), weights[:OUT]),)

    def product(left, value, right):
        return (mm(mm(left, value), right),)

    left, left_next, left_back, packed = local(left_side, 10**9, [square, square, square, (BLOCK // 2, OUT)], factor_in, coupling)
    (right,) = local(lambda factor: (invert(factor),), 2 * 10**9, [full], after(factor_out, long_1))
    right_next, weights = local(right_side, 2 * 10**9, [full, (OUT + BLOCK // 2, OUT)], coupling_out, after(right, long_2), packed)
    (right_back,) = local(lambda right, out: (mm(right, out),), 10**9, [full], after(right, long_3), coupling_out)
    weights = passed_along(weights, 1)
    following = passed_along(gradient, -1)
    (passed,) = local(product, 10**9, [wide], left_back, gradient, right_back)
    back = passed_along(passed, 1)
    (mine,) = local(own_terms, 2 * 10**9, [wide], gradient, left, right, weights)
    (mine,) = local(
        lambda mine, *rest: (mine - product(*rest)[0],), 10**9, [wide], mine, left_next, following, right_next
    )
    return mine - back


def solution(mesh):
    in_specs = (
        P("pipe", "dp", None),
        P("pipe", "dp", None),
        P("pipe", "dp", None),
        P("pipe", None, None),
        P("pipe", "dp", None),
        P("pipe", None, None),
    )
    out_specs = P("pipe", "dp", None)
    return jax.shard_map(shards, mesh=mesh, in_specs=in_specs, out_specs=out_specs, check_vma=False)
```

```python
import jax
import jax.numpy as jnp
from jax import lax
from jax.experimental import pallas as pl
from jax.experimental.pallas import tpu as pltpu
from jax.sharding import PartitionSpec as P


AXES = ("pipe", "dp")
BLOCK = 256
OUT = 512
TOKENS = 256
VMEM = 12 << 20
RING = 8


def permutation(move):
    pairs = []
    for layer in range(16):
        for half in range(2):
            for place in range(RING):
                to_half, to_place = move(layer % 2, half, place)
                pairs.append((layer * 16 + half * RING + place, layer * 16 + to_half % 2 * RING + to_place % RING))
    return pairs


ACROSS = permutation(lambda core, half, place: (half + 1, place))
LONG = permutation(lambda core, half, place: (half, place + (1 if core == 0 else -1)))
SHORT = permutation(lambda core, half, place: (half, place - (1 if core == 0 else -1)))


def passed_along(value, steps):
    first, last = (max(0, -steps), min(16, 16 - steps))
    return lax.ppermute(value, "pipe", [(source, source + steps) for source in range(first, last)])


def mm(left, right, dim=1):
    dims = (((dim,), (0,)), ((), ()))

    def halves(value):
        high = value.astype(jnp.bfloat16)
        return high, (value - high.astype(jnp.float32)).astype(jnp.bfloat16)

    def dot(one, two):
        return lax.dot_general(one, two, dims, preferred_element_type=jnp.float32)

    (left_high, left_low), (right_high, right_low) = halves(left), halves(right)
    return dot(left_high, right_high) + (dot(left_high, right_low) + dot(left_low, right_high))


def invert(factor):
    shape = factor.shape
    twice = jnp.where(lax.broadcasted_iota(jnp.int32, shape, 0) == lax.broadcasted_iota(jnp.int32, shape, 1), 2.0, 0.0)
    scale = 1.0 / jnp.max(jnp.sum(jnp.abs(factor), axis=1, keepdims=True), axis=0, keepdims=True)
    iterate = scale * (twice - scale * factor)
    return mm(iterate, twice - mm(factor, iterate))


def local(body, flops, shapes, *operands):
    def kernel(*refs):
        results = body(*[ref[...] for ref in refs[: len(operands)]])
        for ref, result in zip(refs[len(operands) :], results):
            ref[...] = result

    return pl.pallas_call(
        kernel,
        out_shape=[jax.ShapeDtypeStruct(shape, jnp.float32) for shape in shapes],
        cost_estimate=pl.CostEstimate(flops=flops, transcendentals=0, bytes_accessed=1 << 20),
        compiler_params=pltpu.CompilerParams(vmem_limit_bytes=VMEM),
    )(*operands)


def contract_tokens(left, right):
    return lax.dot_general(left, right, (((0,), (0,)), ((), ())), preferred_element_type=jnp.float32)


def shards(inputs, cotangents, input_factors, output_factors, input_coupling, output_coupling):
    return whole(inputs[0], cotangents[0], input_factors[0], output_factors[0], input_coupling[0], output_coupling[0])[None]


def sent(value, pairs):
    return lax.ppermute(value, AXES, pairs)


def after(value, *events):
    return lax.optimization_barrier((value, *events))[0]


def whole(rows, cots, factor_in, factor_out, coupling, coupling_out):
    def gather(*lists):
        widths = [BLOCK * len(blocks) for blocks in lists]
        count = sum(len(blocks) for blocks in lists)

        def kernel(rows_ref, cots_ref, *refs):
            outs, sems = refs[: len(lists)], refs[len(lists)]
            spot = lax.axis_index("dp")
            half, place = spot // RING, spot % RING
            sign = 1 - 2 * (lax.axis_index("pipe") % 2)
            copies = []
            for out, blocks in zip(outs, lists):
                at = 0
                for block in blocks:
                    if isinstance(block, int):
                        source, width = cots_ref.at[:, block * BLOCK : (block + 1) * BLOCK], BLOCK
                    else:
                        own, offset = block
                        start = (half if own else 1 - half) * (RING * BLOCK) + (place + sign * offset + RING) % RING * BLOCK
                        source, width = rows_ref.at[:, pl.ds(pl.multiple_of(start, BLOCK), BLOCK)], BLOCK
                    copies.append(pltpu.make_async_copy(source, out.at[:, at : at + width], sems.at[len(copies)]))
                    at += width
            for copy in copies:
                copy.start()
            for copy in copies:
                copy.wait()

        return pl.pallas_call(
            kernel,
            out_shape=[jax.ShapeDtypeStruct((TOKENS, width), jnp.bfloat16) for width in widths],
            in_specs=[pl.BlockSpec(memory_space=pltpu.HBM)] * 2,
            out_specs=[pl.BlockSpec(memory_space=pltpu.VMEM) for _ in widths],
            scratch_shapes=[pltpu.SemaphoreType.DMA((count,))],
            cost_estimate=pl.CostEstimate(flops=10**8, transcendentals=0, bytes_accessed=2 * 512 * sum(widths)),
            compiler_params=pltpu.CompilerParams(vmem_limit_bytes=VMEM),
        )(pltpu.with_memory_space_constraint(rows, pltpu.HBM), pltpu.with_memory_space_constraint(cots, pltpu.HBM))

    groups = ((4,), (-3,), (3,), (-2,), (2, -1), (1, 0))
    (message,) = gather([(False, 4), 0])
    arrived = {0: sent(message, ACROSS)}
    *messages, own_4, own_m3, own_3, own_m2, own_5, own_6 = gather(
        [(False, -3)],
        [1],
        *[[(False, offset) for offset in group] for group in groups[2:]],
        *[[(True, offset) for offset in group] for group in groups],
    )
    for index, message in enumerate(messages, 1):
        arrived[index] = sent(message, ACROSS)

    def sums(mine, cots, theirs, their_cots):
        return contract_tokens(mine, cots) + contract_tokens(theirs, their_cots)

    def first(mine, cots, zero):
        return (sums(mine, cots[:, :BLOCK], zero[:, :BLOCK], zero[:, BLOCK:]),)

    def other(mine, cots, zero, theirs):
        return (sums(mine, cots[:, :BLOCK], theirs, zero[:, BLOCK:]),)

    def second(mine_0, mine_1, cots, zero, one, far):
        far_cots = cots[:, BLOCK:]
        return sums(mine_0, far_cots, zero[:, :BLOCK], far), sums(mine_1, far_cots, one, far)

    def later(mine, cots, zero, far, theirs):
        return tuple(
            sums(mine[:, at : at + BLOCK], cots[:, part * BLOCK : (part + 1) * BLOCK], theirs[:, at : at + BLOCK], their_cots)
            for at in range(0, mine.shape[1], BLOCK)
            for part, their_cots in enumerate((zero[:, BLOCK:], far))
        )

    partial = {}
    tile, work = (BLOCK, BLOCK), 4 * BLOCK**3
    partial[4, 0] = local(first, work, [tile], own_4, cots, arrived[0])[0]
    partial[-3, 0] = local(other, work, [tile], own_m3, cots, arrived[0], arrived[1])[0]
    partial[4, 1], partial[-3, 1] = local(
        second, 2 * work, [tile] * 2, own_4, own_m3, cots, arrived[0], arrived[1], arrived[2]
    )
    for index, mine in ((3, own_3), (4, own_m2), (5, own_5), (6, own_6)):
        group = groups[index - 1]
        count = 2 * len(group)
        values = local(later, count * work, [tile] * count, mine, cots, arrived[0], arrived[2], arrived[index])
        for at, offset in enumerate(group):
            partial[offset, 0], partial[offset, 1] = values[2 * at : 2 * at + 2]

    def hop(value, pairs, offset, part):
        value = sent(value, pairs)
        return local(lambda one, two: (one + two,), 10**6, [tile], value, partial[offset, part])[0]

    long_way = [partial[4, 0], partial[4, 1]]
    short_way = [partial[-3, 0], partial[-3, 1]]
    marks = []
    for long_next, short_next in ((3, -2), (2, -1), (1, None)):
        for part in range(2):
            long_way[part] = hop(long_way[part], LONG, long_next, part)
        for part in range(2):
            if short_next is None:
                short_way[part] = sent(short_way[part], SHORT)
            else:
                short_way[part] = hop(short_way[part], SHORT, short_next, part)
        marks.append(long_way[1])
    long_1, long_2, long_3 = marks
    long_way = [sent(long_way[part], LONG) for part in range(2)]

    def whole_gradient(*values):
        return (jnp.concatenate([values[part] + values[2 + part] + values[4 + part] for part in range(2)], axis=1),)

    (gradient,) = local(whole_gradient, 10**6, [(BLOCK, OUT)], *long_way, *short_way, partial[0, 0], partial[0, 1])

    square, wide, full = (BLOCK, BLOCK), (BLOCK, OUT), (OUT, OUT)

    def left_side(factor, coupling):
        left = invert(factor)
        left_next = mm(left, coupling)
        left_own = mm(coupling, left_next, 0)
        packed = jnp.concatenate([left_own[: BLOCK // 2], left_own[BLOCK // 2 :]], axis=1)
        return left, left_next, mm(coupling, left, 0), packed

    def right_side(coupling_out, right, packed):
        right_next = mm(coupling_out, right, 0)
        return right_next, jnp.concatenate([mm(right_next, coupling_out), packed], axis=0)

    def own_terms(gradient, left, right, weights):
        left_own = jnp.concatenate([weights[OUT:, :BLOCK], weights[OUT:, BLOCK:]], axis=0)
        return (mm(mm(left, gradient), right) + mm(mm(left_own, gradient), weights[:OUT]),)

    def product(left, value, right):
        return (mm(mm(left, value), right),)

    left, left_next, left_back, packed = local(left_side, 10**9, [square, square, square, (BLOCK // 2, OUT)], factor_in, coupling)
    (right,) = local(lambda factor: (invert(factor),), 2 * 10**9, [full], after(factor_out, long_1))
    right_next, weights = local(right_side, 2 * 10**9, [full, (OUT + BLOCK // 2, OUT)], coupling_out, after(right, long_2), packed)
    (right_back,) = local(lambda right, out: (mm(right, out),), 10**9, [full], after(right, long_3), coupling_out)
    weights = passed_along(weights, 1)
    following = passed_along(gradient, -1)
    (passed,) = local(product, 10**9, [wide], left_back, gradient, right_back)
    back = passed_along(passed, 1)
    (mine,) = local(own_terms, 2 * 10**9, [wide], gradient, left, right, weights)
    (mine,) = local(
        lambda mine, *rest: (mine - product(*rest)[0],), 10**9, [wide], mine, left_next, following, right_next
    )
    return mine - back


def solution(mesh):
    in_specs = (
        P("pipe", "dp", None),
        P("pipe", "dp", None),
        P("pipe", "dp", None),
        P("pipe", None, None),
        P("pipe", "dp", None),
        P("pipe", None, None),
    )
    out_specs = P("pipe", "dp", None)
    return jax.shard_map(shards, mesh=mesh, in_specs=in_specs, out_specs=out_specs, check_vma=False)
```

```python
import jax
import jax.numpy as jnp
from jax import lax
from jax.experimental import pallas as pl
from jax.experimental.pallas import tpu as pltpu
from jax.sharding import PartitionSpec as P


AXES = ("pipe", "dp")
BLOCK = 256
OUT = 512
TOKENS = 256
VMEM = 12 << 20
RING = 8


def permutation(move):
    pairs = []
    for layer in range(16):
        for half in range(2):
            for place in range(RING):
                to_half, to_place = move(layer % 2, half, place)
                pairs.append((layer * 16 + half * RING + place, layer * 16 + to_half % 2 * RING + to_place % RING))
    return pairs


ACROSS = permutation(lambda core, half, place: (half + 1, place))
LONG = permutation(lambda core, half, place: (half, place + (1 if core == 0 else -1)))
SHORT = permutation(lambda core, half, place: (half, place - (1 if core == 0 else -1)))


def passed_along(value, steps):
    first, last = (max(0, -steps), min(16, 16 - steps))
    return lax.ppermute(value, "pipe", [(source, source + steps) for source in range(first, last)])


def mm(left, right, dim=1):
    dims = (((dim,), (0,)), ((), ()))

    def halves(value):
        high = value.astype(jnp.bfloat16)
        return high, (value - high.astype(jnp.float32)).astype(jnp.bfloat16)

    def dot(one, two):
        return lax.dot_general(one, two, dims, preferred_element_type=jnp.float32)

    (left_high, left_low), (right_high, right_low) = halves(left), halves(right)
    return dot(left_high, right_high) + (dot(left_high, right_low) + dot(left_low, right_high))


def invert(factor):
    shape = factor.shape
    twice = jnp.where(lax.broadcasted_iota(jnp.int32, shape, 0) == lax.broadcasted_iota(jnp.int32, shape, 1), 2.0, 0.0)
    scale = 1.0 / jnp.max(jnp.sum(jnp.abs(factor), axis=1, keepdims=True), axis=0, keepdims=True)
    iterate = scale * (twice - scale * factor)
    return mm(iterate, twice - mm(factor, iterate))


def local(body, flops, shapes, *operands):
    def kernel(*refs):
        results = body(*[ref[...] for ref in refs[: len(operands)]])
        for ref, result in zip(refs[len(operands) :], results):
            ref[...] = result

    return pl.pallas_call(
        kernel,
        out_shape=[jax.ShapeDtypeStruct(shape, jnp.float32) for shape in shapes],
        cost_estimate=pl.CostEstimate(flops=flops, transcendentals=0, bytes_accessed=1 << 20),
        compiler_params=pltpu.CompilerParams(vmem_limit_bytes=VMEM),
    )(*operands)


def contract_tokens(left, right):
    return lax.dot_general(left, right, (((0,), (0,)), ((), ())), preferred_element_type=jnp.float32)


def shards(inputs, cotangents, input_factors, output_factors, input_coupling, output_coupling):
    return whole(inputs[0], cotangents[0], input_factors[0], output_factors[0], input_coupling[0], output_coupling[0])[None]


def sent(value, pairs):
    return lax.ppermute(value, AXES, pairs)


def after(value, *events):
    return lax.optimization_barrier((value, *events))[0]


def whole(rows, cots, factor_in, factor_out, coupling, coupling_out):
    def gather(*lists):
        widths = [BLOCK * len(blocks) for blocks in lists]
        count = sum(len(blocks) for blocks in lists)

        def kernel(rows_ref, cots_ref, *refs):
            outs, sems = refs[: len(lists)], refs[len(lists)]
            spot = lax.axis_index("dp")
            half, place = spot // RING, spot % RING
            sign = 1 - 2 * (lax.axis_index("pipe") % 2)
            copies = []
            for out, blocks in zip(outs, lists):
                at = 0
                for block in blocks:
                    if isinstance(block, int):
                        source, width = cots_ref.at[:, block * BLOCK : (block + 1) * BLOCK], BLOCK
                    else:
                        own, offset = block
                        start = (half if own else 1 - half) * (RING * BLOCK) + (place + sign * offset + RING) % RING * BLOCK
                        source, width = rows_ref.at[:, pl.ds(pl.multiple_of(start, BLOCK), BLOCK)], BLOCK
                    copies.append(pltpu.make_async_copy(source, out.at[:, at : at + width], sems.at[len(copies)]))
                    at += width
            for copy in copies:
                copy.start()
            for copy in copies:
                copy.wait()

        return pl.pallas_call(
            kernel,
            out_shape=[jax.ShapeDtypeStruct((TOKENS, width), jnp.bfloat16) for width in widths],
            in_specs=[pl.BlockSpec(memory_space=pltpu.HBM)] * 2,
            out_specs=[pl.BlockSpec(memory_space=pltpu.VMEM) for _ in widths],
            scratch_shapes=[pltpu.SemaphoreType.DMA((count,))],
            cost_estimate=pl.CostEstimate(flops=10**8, transcendentals=0, bytes_accessed=2 * 512 * sum(widths)),
            compiler_params=pltpu.CompilerParams(vmem_limit_bytes=VMEM),
        )(pltpu.with_memory_space_constraint(rows, pltpu.HBM), pltpu.with_memory_space_constraint(cots, pltpu.HBM))

    groups = ((4,), (-3,), (3,), (-2,), (2, -1), (1, 0))
    (message,) = gather([(False, 4), 0])
    arrived = {0: sent(message, ACROSS)}
    *messages, own_4, own_m3, own_3, own_m2, own_5, own_6 = gather(
        [(False, -3)],
        [1],
        *[[(False, offset) for offset in group] for group in groups[2:]],
        *[[(True, offset) for offset in group] for group in groups],
    )
    for index, message in enumerate(messages, 1):
        arrived[index] = sent(message, ACROSS)

    def sums(mine, cots, theirs, their_cots):
        return contract_tokens(mine, cots) + contract_tokens(theirs, their_cots)

    def first(mine, cots, zero):
        return (sums(mine, cots[:, :BLOCK], zero[:, :BLOCK], zero[:, BLOCK:]),)

    def other(mine, cots, zero, theirs):
        return (sums(mine, cots[:, :BLOCK], theirs, zero[:, BLOCK:]),)

    def second(mine_0, mine_1, cots, zero, one, far):
        far_cots = cots[:, BLOCK:]
        return sums(mine_0, far_cots, zero[:, :BLOCK], far), sums(mine_1, far_cots, one, far)

    def later(mine, cots, zero, far, theirs):
        return tuple(
            sums(mine[:, at : at + BLOCK], cots[:, part * BLOCK : (part + 1) * BLOCK], theirs[:, at : at + BLOCK], their_cots)
            for at in range(0, mine.shape[1], BLOCK)
            for part, their_cots in enumerate((zero[:, BLOCK:], far))
        )

    partial = {}
    tile, work = (BLOCK, BLOCK), 4 * BLOCK**3
    partial[4, 0] = local(first, work, [tile], own_4, cots, arrived[0])[0]
    partial[-3, 0] = local(other, work, [tile], own_m3, cots, arrived[0], arrived[1])[0]
    partial[4, 1], partial[-3, 1] = local(
        second, 2 * work, [tile] * 2, own_4, own_m3, cots, arrived[0], arrived[1], arrived[2]
    )
    for index, mine in ((3, own_3), (4, own_m2), (5, own_5), (6, own_6)):
        group = groups[index - 1]
        count = 2 * len(group)
        values = local(later, count * work, [tile] * count, mine, cots, arrived[0], arrived[2], arrived[index])
        for at, offset in enumerate(group):
            partial[offset, 0], partial[offset, 1] = values[2 * at : 2 * at + 2]

    def hop(value, pairs, offset, part):
        value = sent(value, pairs)
        return local(lambda one, two: (one + two,), 10**6, [tile], value, partial[offset, part])[0]

    long_way = [partial[4, 0], partial[4, 1]]
    short_way = [partial[-3, 0], partial[-3, 1]]
    marks = []
    for long_next, short_next in ((3, -2), (2, -1), (1, None)):
        for part in range(2):
            long_way[part] = hop(long_way[part], LONG, long_next, part)
        for part in range(2):
            if short_next is None:
                short_way[part] = sent(short_way[part], SHORT)
            else:
                short_way[part] = hop(short_way[part], SHORT, short_next, part)
        marks.append(long_way[0])
    long_1, _, long_3 = marks
    long_way = [sent(long_way[part], LONG) for part in range(2)]

    def whole_gradient(*values):
        return (jnp.concatenate([values[part] + values[2 + part] + values[4 + part] for part in range(2)], axis=1),)

    (gradient,) = local(whole_gradient, 10**6, [(BLOCK, OUT)], *long_way, *short_way, partial[0, 0], partial[0, 1])

    square, wide, full = (BLOCK, BLOCK), (BLOCK, OUT), (OUT, OUT)

    def left_side(factor, coupling):
        left = invert(factor)
        left_next = mm(left, coupling)
        left_own = mm(coupling, left_next, 0)
        packed = jnp.concatenate([left_own[: BLOCK // 2], left_own[BLOCK // 2 :]], axis=1)
        return left, left_next, mm(coupling, left, 0), packed

    def right_side(coupling_out, right, packed):
        right_next = mm(coupling_out, right, 0)
        return right_next, jnp.concatenate([mm(right_next, coupling_out), packed], axis=0)

    def own_terms(gradient, left, right, weights):
        left_own = jnp.concatenate([weights[OUT:, :BLOCK], weights[OUT:, BLOCK:]], axis=0)
        return (mm(mm(left, gradient), right) + mm(mm(left_own, gradient), weights[:OUT]),)

    def product(left, value, right):
        return (mm(mm(left, value), right),)

    left, left_next, left_back, packed = local(left_side, 10**9, [square, square, square, (BLOCK // 2, OUT)], factor_in, coupling)
    (right,) = local(lambda factor: (invert(factor),), 2 * 10**9, [full], after(factor_out, long_1))
    right_next, weights = local(right_side, 2 * 10**9, [full, (OUT + BLOCK // 2, OUT)], coupling_out, right, packed)
    (right_back,) = local(lambda right, out: (mm(right, out),), 10**9, [full], after(right, long_3), coupling_out)
    weights = passed_along(weights, 1)
    (passed,) = local(product, 10**9, [wide], left_back, gradient, right_back)
    following = passed_along(after(gradient, passed), -1)
    back = passed_along(passed, 1)
    (mine,) = local(own_terms, 2 * 10**9, [wide], gradient, left, right, weights)
    (mine,) = local(
        lambda mine, *rest: (mine - product(*rest)[0],), 10**9, [wide], mine, left_next, following, right_next
    )
    return mine - back


def solution(mesh):
    in_specs = (
        P("pipe", "dp", None),
        P("pipe", "dp", None),
        P("pipe", "dp", None),
        P("pipe", None, None),
        P("pipe", "dp", None),
        P("pipe", None, None),
    )
    out_specs = P("pipe", "dp", None)
    return jax.shard_map(shards, mesh=mesh, in_specs=in_specs, out_specs=out_specs, check_vma=False)
```
